256 devices in a mesh: dp: 8 (over z), w: 4 (over y), h: 8 (over x, core).
Axes of the slice: x: 4, y: 4, z: 8, core: 2. Of those that a mesh axis runs over, the one named last changes fastest.
Arguments:
- field: float32 [96, 32, 128, 256], P('dp', None, 'h', 'w')
- target: float32 [96, 32, 128, 256], P('dp', None, 'h', 'w')
- lat_weight: float32 [128], P('h')
- leg_fwd: float32 [64, 64, 128], P('w', None, 'h')
- leg_inv: float32 [64, 64, 128], P('w', None, 'h')
- spec_w: float32 [2, 64, 32, 32], replicated
- w_in: bfloat16 [32, 64], replicated
- w_out: bfloat16 [64, 32], replicated
Outputs:
- output 1: float32 [], replicated
- output 2: float32 [96, 32, 128, 256], P('dp', None, 'h', 'w')
- output 3: float32 [2, 64, 32, 32], P(None, 'h')
- output 4: float32 [32, 64], replicated
- output 5: float32 [64, 32], replicated
All inputs are finite; a program needn't handle non-finite values.
Results may differ from the reference program's by a relative error of at most 0.00127219.
Values sent between devices are 32-bit elements.
A program may use at most 768 MiB of HBM per device.

```python
import functools
import jax
import jax.numpy as jnp
from jax import lax

BATCH = 96
CHANNELS = 32
NLAT = 128
NLON = 256
LMAX = 64
NORM_EPS = 1e-5
TOTAL = BATCH * CHANNELS * NLAT * NLON


def setup_inputs(seed: int = 0) -> dict:
    keys = jax.random.split(jax.random.key(seed), 12)
    lat_angle = (jnp.arange(NLAT, dtype=jnp.float32) + 0.5) * (jnp.pi / NLAT) - 0.5 * jnp.pi
    lon_angle = jnp.arange(NLON, dtype=jnp.float32) * (2.0 * jnp.pi / NLON)
    grid_shape = (BATCH, CHANNELS, NLAT, NLON)
    chan_mean = jax.random.normal(keys[0], (1, CHANNELS, 1, 1))
    chan_scale = 0.5 + jax.random.uniform(keys[1], (1, CHANNELS, 1, 1))
    wave_amp = jax.random.normal(keys[2], (BATCH, CHANNELS, 1, 1))
    wave_phase = 2.0 * jnp.pi * jax.random.uniform(keys[3], (BATCH, CHANNELS, 1, 1))
    wave = wave_amp * jnp.sin(2.0 * lat_angle)[:, None] * jnp.cos(lon_angle + wave_phase)
    field = chan_mean + chan_scale * (jax.random.normal(keys[4], grid_shape) + wave)
    target = chan_mean + 0.7 * jax.random.normal(keys[5], grid_shape)
    lat_weight = jnp.cos(lat_angle) * (0.5 + jax.random.uniform(keys[6], (NLAT,)))
    degrees = jnp.arange(LMAX)
    tri_mask = (degrees[None, :, None] >= degrees[:, None, None]).astype(jnp.float32)
    leg_fwd = jax.random.normal(keys[7], (LMAX, LMAX, NLAT)) * tri_mask * (NLAT ** -0.5)
    leg_inv = jax.random.normal(keys[8], (LMAX, LMAX, NLAT)) * tri_mask * ((2.0 / LMAX) ** 0.5)
    spec_w = jax.random.normal(keys[9], (2, LMAX, CHANNELS, CHANNELS)) * ((2.0 * CHANNELS) ** -0.5)
    w_in = jax.random.normal(keys[10], (CHANNELS, 2 * CHANNELS)) * (CHANNELS ** -0.5)
    w_out = jax.random.normal(keys[11], (2 * CHANNELS, CHANNELS)) * ((2.0 * CHANNELS) ** -0.5)
    return {"field": field.astype(jnp.float32), "target": target.astype(jnp.float32), "lat_weight": lat_weight.astype(jnp.float32), "leg_fwd": leg_fwd.astype(jnp.float32), "leg_inv": leg_inv.astype(jnp.float32), "spec_w": spec_w.astype(jnp.float32), "w_in": w_in.astype(jnp.bfloat16), "w_out": w_out.astype(jnp.bfloat16)}


def as_bf16_value(values):
    return values + lax.stop_gradient(values.astype(jnp.bfloat16).astype(jnp.float32) - values)


def sample_energy(sample, lat_weight, leg_fwd, leg_inv, spec_w, w_in, w_out):
    field, target = sample
    chan_mean = jnp.mean(field, axis=(1, 2), keepdims=True)
    centred = field - chan_mean
    variance = jnp.mean(centred * centred, axis=(1, 2), keepdims=True)
    normed = centred * lax.rsqrt(variance + NORM_EPS)
    lon_spec = jnp.fft.rfft(normed, axis=2, norm="ortho")[:, :, :LMAX]
    coef_re = jnp.einsum("mlt,ctm->clm", leg_fwd, lon_spec.real)
    coef_im = jnp.einsum("mlt,ctm->clm", leg_fwd, lon_spec.imag)
    mix_re = jnp.einsum("ilm,lio->olm", coef_re, spec_w[0]) - jnp.einsum("ilm,lio->olm", coef_im, spec_w[1])
    mix_im = jnp.einsum("ilm,lio->olm", coef_re, spec_w[1]) + jnp.einsum("ilm,lio->olm", coef_im, spec_w[0])
    back_re = jnp.einsum("mlt,clm->ctm", leg_inv, mix_re)
    back_im = jnp.einsum("mlt,clm->ctm", leg_inv, mix_im)
    back_spec = jnp.pad(lax.complex(back_re, back_im), ((0, 0), (0, 0), (0, NLON // 2 + 1 - LMAX)))
    y_grid = jnp.fft.irfft(back_spec, n=NLON, axis=2, norm="ortho")
    hidden = jnp.einsum("ctp,cf->ftp", as_bf16_value(y_grid), w_in)
    activation = as_bf16_value(jax.nn.gelu(hidden))
    mlp_out = jnp.einsum("ftp,fc->ctp", activation, w_out)
    residual = field + y_grid + mlp_out - target
    return 0.5 * jnp.sum(lat_weight[:, None] * residual * residual)


def total_energy(field, spec_w, w_in, w_out, target, lat_weight, leg_fwd, leg_inv):
    body = jax.checkpoint(functools.partial(sample_energy, lat_weight=lat_weight, leg_fwd=leg_fwd, leg_inv=leg_inv, spec_w=spec_w, w_in=w_in, w_out=w_out))
    return jnp.sum(lax.map(body, (field, target)))


def reference(field, target, lat_weight, leg_fwd, leg_inv, spec_w, w_in, w_out):
    energy_fn = functools.partial(total_energy, target=target, lat_weight=lat_weight, leg_fwd=leg_fwd, leg_inv=leg_inv)
    energy, pullback = jax.vjp(energy_fn, field, spec_w, w_in.astype(jnp.float32), w_out.astype(jnp.float32))
    grad_field, grad_spec, grad_w_in, grad_w_out = pullback(jnp.ones_like(energy))
    loss = 2.0 * energy / TOTAL
    return (loss, grad_field, grad_spec, grad_w_in, grad_w_out)
```

```python
import functools
import numpy as np
import jax
import jax.numpy as jnp
from jax import lax
from jax.experimental import pallas as pl
from jax.experimental.pallas import tpu as pltpu
from jax.sharding import PartitionSpec as P

NORM_EPS = 1e-5
HI = lax.Precision.HIGHEST
GELU_C = 0.7978845608028654
GELU_A = 0.044715
NT = (((1,), (1,)), ((), ()))
NN = (((1,), (0,)), ((), ()))
F32 = jnp.float32
LANES, HALF_LANES, CHANS, ROWS = 128, 64, 32, 256
BF16 = jnp.bfloat16


def dot(a, b, dims, precision=HI):
    return lax.dot_general(a, b, dims, precision=precision, preferred_element_type=F32)


def dft_tables(nlon, modes, w_size, h_size):
    per = modes // (w_size * h_size)
    order = [w * (modes // w_size) + h * per + j for h in range(h_size) for w in range(w_size) for j in range(per)]
    m = np.array(order)[:, None]
    n = np.arange(nlon)[None, :]
    ang = 2.0 * np.pi * ((m * n) % nlon) / nlon
    fwd = np.concatenate([np.cos(ang), -np.sin(ang)]) / np.sqrt(nlon)
    mult = np.where(m == 0, 1.0, 2.0)
    inv = np.concatenate([mult * np.cos(ang), -mult * np.sin(ang)]) / np.sqrt(nlon)
    lon = nlon // w_size

    def spread(t):
        out = np.zeros((2, 2 * modes, w_size, 2, lon))
        for half in range(2):
            out[half, :, :, half, :] = t.reshape(2 * modes, w_size, lon)
        return out.reshape(4 * modes, 2 * nlon).astype(np.float32)

    return spread(fwd), spread(inv)

GROUPS = 3
MESH = pl.DeviceIdType.MESH


class Links:
    def __init__(self, send_sem, recv_sem):
        self.h, self.w, self.dp = lax.axis_index("h"), lax.axis_index("w"), lax.axis_index("dp")
        self.me = self.h * 4 + self.w
        self.send_sem, self.recv_sem = send_sem, recv_sem
        self.sent = []

    def plane_device(self, i):
        k = i + 1
        chip = lax.rem(5 * lax.rem(k, 16), 16)
        x = lax.rem(self.h // 2 + lax.rem(chip, 4), 4)
        w = lax.rem(self.w + chip // 4, 4)
        h = x * 2 + lax.rem(self.h + k // 16, 2)
        return h * 4 + w, {"h": h, "w": w}

    def axis_device(self, axis, n, i):
        t = lax.rem(getattr(self, axis) + 1 + i, n)
        return t, {axis: t}

    def greet(self):
        bar = pltpu.get_barrier_semaphore()

        def plane(i, c):
            pl.semaphore_signal(bar, inc=1, device_id=self.plane_device(i)[1], device_id_type=MESH)
            return c

        def depth(i, c):
            pl.semaphore_signal(bar, inc=1, device_id=self.axis_device("dp", 8, i)[1], device_id_type=MESH)
            return c

        lax.fori_loop(0, 31, plane, 0)
        lax.fori_loop(0, 7, depth, 0)
        pl.semaphore_wait(bar, 38)

    def start(self, src, dst, slot, dev):
        pltpu.make_async_remote_copy(
            src_ref=src, dst_ref=dst, send_sem=self.send_sem.at[slot], recv_sem=self.recv_sem.at[slot],
            device_id=dev, device_id_type=MESH).start()

    def plane_send(self, src, dst, g, rows, stage):
        mine = pl.ds(pl.multiple_of(self.me * rows, rows), rows)

        def one(i, c):
            t, dev = self.plane_device(i)
            theirs = pl.ds(pl.multiple_of(t * rows, rows), rows)
            self.start(src.at[g, theirs], dst.at[g, mine], stage * GROUPS + g, dev)
            return c

        lax.fori_loop(0, 31, one, 0)
        dst[g, mine, :] = src[g, mine, :]

    def plane_wait(self, dst, g, rows, stage, sem=None):
        part = dst.at[g, pl.ds(0, 31 * rows)]
        pltpu.make_async_copy(part, part, (self.recv_sem if sem is None else sem).at[stage * GROUPS + g]).wait()

    def axis_send(self, src_of, dst, axis, n, slot):
        def one(i, c):
            t, dev = self.axis_device(axis, n, i)
            self.start(src_of(t), dst.at[getattr(self, axis)], slot, dev)
            return c

        lax.fori_loop(0, n - 1, one, 0)

    def axis_wait(self, dst, n, slot, sem=None):
        part = dst.at[pl.ds(0, n - 1)]
        pltpu.make_async_copy(part, part, (self.recv_sem if sem is None else sem).at[slot]).wait()


def half_sums(row, low):
    a = jnp.sum(jnp.where(low, row, 0.0), axis=-1, keepdims=True)
    b = jnp.sum(jnp.where(low, 0.0, row), axis=-1, keepdims=True)
    return jnp.where(low, a, b)


def lane_low(shape):
    return lax.broadcasted_iota(jnp.int32, shape, len(shape) - 1) < HALF_LANES


def total(v):
    return jnp.sum(v.reshape(512, LANES), axis=0, keepdims=True)


def dft_stage(x_ref, g, m_ref, d_ref, st_ref):
    low = lane_low((1, LANES))
    v_all = x_ref[g].reshape(8, 4, 2, 16, LANES)
    cols = []
    for j in range(2):
        v = v_all[:, :, j]
        if st_ref is not None:
            mean = half_sums(total(v), low) * (1.0 / 32768.0)
            v = v - mean.reshape(1, 1, 1, LANES)
            var = half_sums(total(v * v), low) * (1.0 / 32768.0)
            inv = lax.rsqrt(var + NORM_EPS)
            v = v * inv.reshape(1, 1, 1, LANES)
            st_ref[g, j:j + 1, :] = mean
            st_ref[g, j + 4:j + 5, :] = inv
        cols.append(jnp.concatenate([v[:, w].reshape(LANES, LANES) for w in range(4)], axis=1))
    out = dot(m_ref[...], jnp.concatenate(cols, axis=0), NT)
    for half in range(2):
        for part in range(2):
            r0 = (half * 2 + part) * HALF_LANES
            for j in range(2):
                d_ref[g, pl.ds(part * 4 + j * 2 + half, HALF_LANES, stride=8), :] = out[r0:r0 + HALF_LANES, j * LANES:(j + 1) * LANES]


def idft_rows(z_ref, g, j, m_ref):
    parts = [z_ref[g, pl.ds(part * 4 + j * 2 + half, HALF_LANES, stride=8), :] for half in range(2) for part in range(2)]
    return dot(jnp.concatenate(parts, axis=0).T, m_ref[...], NN)


def join_grid(cols):
    per_j = [jnp.concatenate([c.reshape(8, 1, 16, LANES) for c in cols[j]], axis=1).reshape(8, 4, 1, 16, LANES) for j in range(2)]
    return jnp.concatenate(per_j, axis=2).reshape(1024, LANES)


def idft_stage(z_ref, g, m_ref, y_ref):
    cols = []
    for j in range(2):
        y = idft_rows(z_ref, g, j, m_ref)
        cols.append([y[:, w * LANES:(w + 1) * LANES] for w in range(4)])
    y_ref[g] = join_grid(cols)


def norm_back_stage(z_ref, g, m_ref, x_ref, st_ref, o_ref):
    low = lane_low((1, LANES))
    x_all = x_ref[g].reshape(8, 4, 2, 16, LANES)
    cols = []
    for j in range(2):
        y = idft_rows(z_ref, g, j, m_ref)
        mean, inv = st_ref[g, j:j + 1, :], st_ref[g, j + 4:j + 5, :]
        xs, ys, s0, s1 = [], [], 0.0, 0.0
        for w in range(4):
            yw = y[:, w * LANES:(w + 1) * LANES]
            xw = (x_all[:, w, j].reshape(LANES, LANES) - mean) * inv
            s0 = s0 + jnp.sum(yw, axis=0, keepdims=True)
            s1 = s1 + jnp.sum(yw * xw, axis=0, keepdims=True)
            xs.append(xw)
            ys.append(yw)
        s0 = half_sums(s0, low) * (1.0 / 32768.0)
        s1 = half_sums(s1, low) * (1.0 / 32768.0)
        cols.append([inv * (ys[w] - s0 - xs[w] * s1) for w in range(4)])
    o_ref[g] = join_grid(cols)


def swap_signed(t, top_sign):
    sub = lax.broadcasted_iota(jnp.int32, (8, LANES), 0)
    return jnp.where(sub < 4, top_sign, -top_sign) * pltpu.roll(t, 4, 0)


def to_degrees(x_ref, g, tab_ref):
    x = x_ref[g].reshape(CHANS, 2, 8, LANES)
    x = jnp.concatenate([x[:, 0].reshape(ROWS, LANES), x[:, 1].reshape(ROWS, LANES)], axis=1)
    return dot(x, tab_ref[...], NN)


def from_degrees(b, tab_ref, o_ref, g):
    y = dot(b, tab_ref[...], NT)
    y = jnp.concatenate([y[:, :LANES].reshape(CHANS, 1, 8, LANES), y[:, LANES:].reshape(CHANS, 1, 8, LANES)], axis=1)
    o_ref[g] = y.reshape(512, LANES)


def mix(src_ref, g, k_ref, dst_ref, adjoint):
    sign = 1.0 if adjoint else -1.0

    def body(c, acc):
        a = src_ref[g, pl.ds(pl.multiple_of(c * 8, 8), 8), :]
        s = swap_signed(a, sign)
        new = []
        for o in range(CHANS):
            if adjoint:
                kr, ki = k_ref[0, o, pl.ds(c, 1), :], k_ref[1, o, pl.ds(c, 1), :]
            else:
                kr, ki = k_ref[0, c, o:o + 1, :], k_ref[1, c, o:o + 1, :]
            new.append(acc[o] + (a * kr + s * ki))
        return tuple(new)

    acc = lax.fori_loop(0, CHANS, body, tuple(jnp.zeros((8, LANES), F32) for _ in range(CHANS)))
    for o in range(CHANS):
        dst_ref[o * 8:(o + 1) * 8, :] = acc[o]


def row_sums(v):
    sub = lax.broadcasted_iota(jnp.int32, (8, LANES), 0)
    low = sub < 4
    u = [jnp.where(low, v[j], v[j + 4]) + pltpu.roll(jnp.where(low, v[j + 4], v[j]), 4, 0) for j in range(4)]
    for step, n in ((2, 2), (1, 1)):
        first = lax.rem(sub // step, 2) == 0
        u = [jnp.where(first, u[j] + pltpu.roll(u[j], 8 - step, 0), u[j + n] + pltpu.roll(u[j + n], step, 0)) for j in range(n)]
    return u[0]


def kernel_grad(a_ref, d_ref, s_ref, gk_ref):
    def turn(o, carry):
        at = pl.ds(pl.multiple_of(o * 8, 8), 8)
        for g in range(GROUPS):
            s_ref[g, at, :] = swap_signed(d_ref[g, at, :], 1.0)
        return carry

    lax.fori_loop(0, CHANS, turn, 0)

    def rows(c, carry):
        at = pl.ds(pl.multiple_of(c * 8, 8), 8)
        a = [a_ref[g, at, :] for g in range(GROUPS)]
        for blk in range(4):
            for q, ref in ((0, d_ref), (1, s_ref)):
                prods = []
                for o in range(blk * 8, blk * 8 + 8):
                    prods.append(sum(a[g] * ref[g, o * 8:(o + 1) * 8, :] for g in range(GROUPS)))
                gk_ref[q, pl.ds(pl.multiple_of(c * CHANS + blk * 8, 8), 8), :] = row_sums(prods)
        return carry

    lax.fori_loop(0, CHANS, rows, 0)


def mlp_stage(y_ref, x_ref, t_ref, g, q, w1, w2, w1t, w2t, dy_ref, do_ref, sm_ref):
    for j in range(2):
        def take(ref):
            return jnp.concatenate([ref[g, pl.ds(j * 16 + r, CHANS, stride=CHANS), :] for r in range(16)], axis=1)

        y = take(y_ref)
        y_bf = y.astype(BF16)
        hid = dot(w1t, y_bf, NN, None)
        th = jnp.tanh(GELU_C * (hid + GELU_A * (hid * hid * hid)))
        cdf = 0.5 * (1.0 + th)
        act = (hid * cdf).astype(BF16)
        dgelu = cdf + (0.5 * hid * (1.0 - th * th)) * (GELU_C * (1.0 + (3.0 * GELU_A) * (hid * hid)))
        res = take(x_ref) + y + dot(w2t, act, NN, None) - take(t_ref)
        d_out = q * res
        sq = jnp.sum(d_out * res, axis=0, keepdims=True)
        sm_ref[CHANS:33, :] += sum(sq[:, r * LANES:(r + 1) * LANES] for r in range(16))
        d_bf = d_out.astype(BF16)
        g2 = dot(d_bf, act, NT, None)
        d_hid = (dot(w2, d_bf, NN, None) * dgelu).astype(BF16)
        g1 = dot(y_bf, d_hid, NT, None)
        sm_ref[0:CHANS, :] += jnp.concatenate([g1, g2], axis=1)
        d_y = d_out + dot(w1, d_hid, NN, None)
        for r in range(16):
            rows = pl.ds(j * 16 + r, CHANS, stride=CHANS)
            do_ref[g, rows, :] = d_out[:, r * LANES:(r + 1) * LANES]
            dy_ref[g, rows, :] = d_y[:, r * LANES:(r + 1) * LANES]


def pack_stage(x_ref, g, o_ref):
    parts = [jnp.concatenate([x_ref[g * 2 + j], x_ref[g * 2 + j + 6]], axis=-1) for j in range(2)]
    o_ref[g] = jnp.concatenate(parts, axis=1).reshape(1024, LANES)


BIG, HALF, SMALL = CHANS, 16, 40
EXTRA = 8 * GROUPS
(TAB, SM_A, SM_B, SM_C, GK_A, GK_B, GK_C) = range(EXTRA, EXTRA + 7)


def block_kernel(x_hbm, t_hbm, q_ref, w1_ref, w2t_ref, lp_ref, lq_ref, k_hbm, gf_hbm, gi_hbm,
                 out_hbm, gs_ref, smo_ref,
                 x_ref, t_ref, kw_ref, k_ref, gf_ref, gi_ref, q_row, tab,
                 s1, r1, s2, r2, s3, r3, s4, r4, s5, r5, s6, r6, s7, r7, s8, r8, tg, do,
                 st, acc_a, acc_d, acc_s, mixed, tabs, tp, tq, gk, gkt, gr1, gp, gr2, go, sm, sma, smb, smc, sb, sc,
                 send_sem, recv_sem, load_sem):
    links = Links(send_sem, recv_sem)
    low = lane_low((LANES, LANES))

    def load(src, dst, g, half):
        at = pl.ds(g * 2 + half * 6, 2)
        return pltpu.make_async_copy(src.at[at], dst.at[at], load_sem.at[(src is t_hbm) * 6 + g * 2 + half])

    for src, dst in ((x_hbm, x_ref), (t_hbm, t_ref)):
        for g in range(GROUPS):
            load(src, dst, g, 0).start()
            load(src, dst, g, 1).start()
        if src is x_hbm:
            tables = [pltpu.make_async_copy(a, b, load_sem.at[12 + i]) for i, (a, b) in enumerate(((gf_hbm, gf_ref), (k_hbm, kw_ref), (gi_hbm, gi_ref)))]
            for copy in tables:
                copy.start()
    links.greet()

    def groups(fn):
        def one(g, c):
            fn(g)
            return c

        lax.fori_loop(0, GROUPS, one, 0)

    def first(g):
        load(x_hbm, x_ref, g, 0).wait()
        load(x_hbm, x_ref, g, 1).wait()
        pack_stage(x_ref, g, s1)
        links.plane_send(s1, r1, g, BIG, 0)

    groups(first)
    for q, ref in ((0, lp_ref), (1, lq_ref)):
        for i in range(8):
            tab[i, q * 16:(q + 1) * 16, :] = jnp.concatenate([ref[2 * i], ref[2 * i + 1]], axis=1)
    links.axis_send(lambda t: tab.at[t], tabs, "h", 8, TAB)
    tabs[links.h] = tab[links.h]
    for r in range(16):
        q_row[:, r * LANES:(r + 1) * LANES] = jnp.full((1, LANES), q_ref[r], F32)
    for copy in tables:
        copy.wait()

    def widen(c, carry):
        for part in range(2):
            k_ref[part, c] = jnp.concatenate([kw_ref[part, c], kw_ref[part, c]], axis=1)
        return carry

    lax.fori_loop(0, CHANS, widen, 0)

    def take_target(g):
        load(t_hbm, t_ref, g, 0).wait()
        load(t_hbm, t_ref, g, 1).wait()
        pack_stage(t_ref, g, tg)

    groups(take_target)
    sm[...] = jnp.zeros((SMALL, LANES), F32)
    links.axis_wait(tabs, 8, TAB)
    for q, ref in ((0, tp), (1, tq)):
        rows = tabs[:, q * 16:(q + 1) * 16, :].reshape(LANES, LANES)
        ref[0:LANES, :] = jnp.where(low, rows, 0.0)
        ref[LANES:ROWS, :] = jnp.where(low, 0.0, rows)

    def second(g):
        links.plane_wait(r1, g, BIG, 0)
        dft_stage(r1, g, gf_ref, s2, st)
        links.plane_send(s2, r2, g, HALF, 1)

    def third(g):
        links.plane_wait(r2, g, HALF, 1)
        acc_a[g] = to_degrees(r2, g, tp)
        mix(acc_a, g, k_ref, mixed, False)
        from_degrees(mixed[...], tq, s3, g)
        links.plane_send(s3, r3, g, HALF, 2)

    def fourth(g):
        links.plane_wait(r3, g, HALF, 2)
        idft_stage(r3, g, gi_ref, s4)
        links.plane_send(s4, r4, g, BIG, 3)

    w1, w2t = w1_ref[...], w2t_ref[...]
    w1t, w2 = w1.astype(F32).T.astype(BF16), w2t.astype(F32).T.astype(BF16)

    def fifth(g):
        links.plane_wait(r4, g, BIG, 3)
        mlp_stage(r4, s1, tg, g, q_row[...], w1, w2, w1t, w2t, s5, do, sm)
        links.plane_send(s5, r5, g, BIG, 4)

    def sixth(g):
        links.plane_wait(r5, g, BIG, 4)
        dft_stage(r5, g, gi_ref, s6, None)
        links.plane_send(s6, r6, g, HALF, 5)

    def seventh(g):
        links.plane_wait(r6, g, HALF, 5)
        acc_d[g] = to_degrees(r6, g, tq)
        mix(acc_d, g, k_ref, mixed, True)
        from_degrees(mixed[...], tp, s7, g)
        links.plane_send(s7, r7, g, HALF, 6)

    def eighth(g):
        links.plane_wait(r7, g, HALF, 6)
        norm_back_stage(r7, g, gf_ref, r1, st, s8)
        links.plane_send(s8, r8, g, BIG, 7)

    def ninth(g):
        links.plane_wait(r8, g, BIG, 7)
        do[g] = do[g] + r8[g]
        pltpu.make_async_copy(do.at[g], out_hbm.at[g], load_sem.at[15 + g]).start()

    for stage in (second, third, fourth, fifth):
        groups(stage)

    links.axis_send(lambda t: sm, sma, "dp", 8, SM_A)
    sma[links.dp] = sm[...]
    groups(sixth)
    links.axis_wait(sma, 8, SM_A)
    sb[...] = jnp.sum(sma[...], axis=0)
    links.axis_send(lambda t: sb, smb, "h", 8, SM_B)
    smb[links.h] = sb[...]
    groups(seventh)
    links.axis_wait(smb, 8, SM_B)
    sc[...] = jnp.sum(smb[...], axis=0)
    links.axis_send(lambda t: sc, smc, "w", 4, SM_C)
    smc[links.w] = sc[...]


    kernel_grad(acc_a, acc_d, acc_s, gk)

    def turn(n, c):
        for q in range(2):
            t = gk[q, pl.ds(pl.multiple_of(n * LANES, LANES), LANES), :].T
            i = q * 8 + n
            gkt[i // 2, pl.ds(pl.multiple_of(lax.rem(i, 2) * HALF_LANES, HALF_LANES), HALF_LANES), :] = t[0:HALF_LANES] + t[HALF_LANES:LANES]
        return c

    lax.fori_loop(0, 8, turn, 0)
    links.axis_send(lambda t: gkt.at[t], gr1, "dp", 8, GK_A)
    gr1[links.dp] = gkt[links.dp]
    eighth(0)
    eighth(1)
    links.axis_wait(gr1, 8, GK_A)
    part = jnp.sum(gr1[...], axis=0)
    for n in range(2):
        gp[:, n * 8:(n + 1) * 8, :] = part[n * HALF_LANES:(n + 1) * HALF_LANES].reshape(8, 8, LANES)

    def spread(i, c):
        t, dev = links.plane_device(i)
        links.start(gp.at[t // 4], gr2.at[links.me], GK_B, dev)
        return c

    lax.fori_loop(0, 31, spread, 0)
    gr2[links.me] = gp[links.h]
    eighth(2)
    ninth(0)
    links.axis_wait(gr2, CHANS, GK_B)
    go[...] = jnp.sum(gr2[...], axis=0)
    links.axis_send(lambda t: go, gs_ref, "dp", 8, GK_C)
    gs_ref[links.dp] = go[...]
    links.axis_wait(smc, 4, SM_C)
    smo_ref[...] = jnp.sum(smc[...], axis=0)
    ninth(1)
    ninth(2)
    links.axis_wait(gs_ref, 8, GK_C)
    for g in range(GROUPS):
        pltpu.make_async_copy(do.at[g], out_hbm.at[g], load_sem.at[15 + g]).wait()

    for stage, (buf, rows) in enumerate(((s1, BIG), (s2, HALF), (s3, HALF), (s4, BIG), (s5, BIG), (s6, HALF), (s7, HALF), (s8, BIG))):
        groups(lambda g, buf=buf, rows=rows, stage=stage: links.plane_wait(buf, g, rows, stage, send_sem))
    for buf, n, slot in ((tabs, 8, TAB), (sma, 8, SM_A), (smb, 8, SM_B), (smc, 4, SM_C), (gr1, 8, GK_A), (gr2, CHANS, GK_B), (gs_ref, 8, GK_C)):
        links.axis_wait(buf, n, slot, send_sem)


def run_block(*args):
    big, half = pltpu.VMEM((GROUPS, 1024, LANES), F32), pltpu.VMEM((GROUPS, 512, LANES), F32)
    stages = [big, big, half, half, half, half, big, big, big, big, half, half, half, half, big, big, big, big]
    vm = lambda *s: pltpu.VMEM(s, F32)
    fields = [vm(12, CHANS, 16, HALF_LANES), vm(12, CHANS, 16, HALF_LANES), vm(2, CHANS, CHANS, HALF_LANES), vm(2, CHANS, CHANS, LANES), vm(ROWS, 512), vm(ROWS, 512), vm(1, 2048), vm(8, CHANS, LANES)]
    scratch = fields + stages + [
        vm(GROUPS, 8, LANES), vm(GROUPS, ROWS, LANES), vm(GROUPS, ROWS, LANES), vm(GROUPS, ROWS, LANES), vm(ROWS, LANES),
        vm(8, CHANS, LANES), vm(ROWS, LANES), vm(ROWS, LANES),
        vm(2, 1024, LANES), vm(8, LANES, LANES), vm(8, LANES, LANES), vm(8, 16, LANES), vm(CHANS, 16, LANES), vm(16, LANES),
        vm(SMALL, LANES), vm(8, SMALL, LANES), vm(8, SMALL, LANES), vm(4, SMALL, LANES), vm(SMALL, LANES), vm(SMALL, LANES),
        pltpu.SemaphoreType.DMA((EXTRA + 7,)), pltpu.SemaphoreType.DMA((EXTRA + 7,)), pltpu.SemaphoreType.DMA((18,)),
    ]
    space, hbm = pl.BlockSpec(memory_space=pltpu.VMEM), pl.BlockSpec(memory_space=pl.ANY)
    return pl.pallas_call(
        block_kernel,
        out_shape=[
            jax.ShapeDtypeStruct((GROUPS, 1024, LANES), F32),
            jax.ShapeDtypeStruct((8, 16, LANES), F32),
            jax.ShapeDtypeStruct((SMALL, LANES), F32),
        ],
        in_specs=[hbm, hbm, pl.BlockSpec(memory_space=pltpu.SMEM), space, space, space, space, hbm, hbm, hbm],
        out_specs=[hbm, space, space],
        scratch_shapes=scratch,
        compiler_params=pltpu.CompilerParams(collective_id=0, has_side_effects=True, vmem_limit_bytes=62 * 1024 * 1024),
        name="block",
    )(*args)


def unpack_kernel(v_ref, o_ref):
    for j in range(2):
        v = v_ref[0, :, j * 16:(j + 1) * 16, :]
        o_ref[0, j] = v[:, :, :HALF_LANES]
        o_ref[1, j] = v[:, :, HALF_LANES:]


def unpack(v):
    return pl.pallas_call(
        unpack_kernel,
        grid=(GROUPS,),
        in_specs=[pl.BlockSpec((1, CHANS, CHANS, LANES), lambda g: (g, 0, 0, 0))],
        out_specs=pl.BlockSpec((2, 2, CHANS, 16, HALF_LANES), lambda g: (0, g, 0, 0, 0)),
        out_shape=jax.ShapeDtypeStruct((2, 6, CHANS, 16, HALF_LANES), F32),
        name="unpack",
    )(v.reshape(GROUPS, CHANS, CHANS, LANES)).reshape(12, CHANS, 16, HALF_LANES)


def solution(mesh):
    w_size, h_size, dp_size = mesh.shape["w"], mesh.shape["h"], mesh.shape["dp"]
    fwd_np, inv_np = dft_tables(ROWS, HALF_LANES, w_size, h_size)

    def local_step(field, target, lat_weight, leg_fwd, leg_inv, spec_w, w_in, w_out):
        gf, gi = jnp.asarray(fwd_np), jnp.asarray(inv_np)
        packed, gs, sm = run_block(
            field, target, lat_weight, w_in, w_out.T, leg_fwd.transpose(0, 2, 1), leg_inv.transpose(0, 2, 1),
            spec_w.transpose(0, 2, 3, 1), gf, gi)
        d_field = unpack(packed)
        grad_spec = gs.reshape(2, 4, 2, 8, 4, CHANS).transpose(0, 3, 1, 2, 4, 5).reshape(2, 8, CHANS, CHANS)
        grad_w_in = sm[:CHANS, :HALF_LANES]
        grad_w_out = sm[:CHANS, HALF_LANES:].T
        loss = jnp.sum(sm[CHANS]) / (dp_size * 384 * 32768)
        return loss, d_field, grad_spec, grad_w_in, grad_w_out

    grid_spec = P("dp", None, "h", "w")
    table_spec = P("w", None, "h")
    kernel_out = P(None, "h", None, None)
    return jax.shard_map(local_step, mesh=mesh, in_specs=(grid_spec, grid_spec, P("h"), table_spec, table_spec, P(), P(), P()), out_specs=(P(), grid_spec, kernel_out, P(), P()), check_vma=False)
```

```python
import functools
import numpy as np
import jax
import jax.numpy as jnp
from jax import lax
from jax.experimental import pallas as pl
from jax.experimental.pallas import tpu as pltpu
from jax.sharding import PartitionSpec as P

NORM_EPS = 1e-5
HI = lax.Precision.HIGHEST
GELU_C = 0.7978845608028654
GELU_A = 0.044715
NT = (((1,), (1,)), ((), ()))
NN = (((1,), (0,)), ((), ()))
F32 = jnp.float32
LANES, HALF_LANES, CHANS, ROWS = 128, 64, 32, 256
BF16 = jnp.bfloat16


def dot(a, b, dims, precision=HI):
    return lax.dot_general(a, b, dims, precision=precision, preferred_element_type=F32)


def dft_tables(nlon, modes, w_size, h_size):
    per = modes // (w_size * h_size)
    order = [w * (modes // w_size) + h * per + j for h in range(h_size) for w in range(w_size) for j in range(per)]
    m = np.array(order)[:, None]
    n = np.arange(nlon)[None, :]
    ang = 2.0 * np.pi * ((m * n) % nlon) / nlon
    fwd = np.concatenate([np.cos(ang), -np.sin(ang)]) / np.sqrt(nlon)
    mult = np.where(m == 0, 1.0, 2.0)
    inv = np.concatenate([mult * np.cos(ang), -mult * np.sin(ang)]) / np.sqrt(nlon)
    lon = nlon // w_size

    def spread(t):
        out = np.zeros((2, 2 * modes, w_size, 2, lon))
        for half in range(2):
            out[half, :, :, half, :] = t.reshape(2 * modes, w_size, lon)
        return out.reshape(4 * modes, 2 * nlon).astype(np.float32)

    return spread(fwd), spread(inv)

GROUPS = 3
MESH = pl.DeviceIdType.MESH


CHIPS = [int(d, 16) for d in "5af49e38d27c16b"]


class Links:
    def __init__(self, send_sem, recv_sem):
        self.h, self.w, self.dp = lax.axis_index("h"), lax.axis_index("w"), lax.axis_index("dp")
        self.me = self.h * 4 + self.w
        self.send_sem, self.recv_sem = send_sem, recv_sem
        self.others = [self.plane_device(i) for i in range(31)]

    def plane_device(self, i):
        chip, core = (CHIPS[i], 0) if i < 15 else ((0, *CHIPS)[i - 15], 1)
        x = lax.rem(self.h // 2 + chip % 4, 4)
        w = lax.rem(self.w + chip // 4, 4)
        h = x * 2 + lax.rem(self.h + core, 2)
        return h * 4 + w, {"h": h, "w": w}

    def axis_device(self, axis, n, i):
        t = lax.rem(getattr(self, axis) + 1 + i, n)
        return t, {axis: t}

    def greet(self):
        bar = pltpu.get_barrier_semaphore()

        def depth(i, c):
            pl.semaphore_signal(bar, inc=1, device_id=self.axis_device("dp", 8, i)[1], device_id_type=MESH)
            return c

        for _, dev in self.others:
            pl.semaphore_signal(bar, inc=1, device_id=dev, device_id_type=MESH)
        lax.fori_loop(0, 7, depth, 0)
        pl.semaphore_wait(bar, 38)

    def start(self, src, dst, slot, dev):
        pltpu.make_async_remote_copy(
            src_ref=src, dst_ref=dst, send_sem=self.send_sem.at[slot], recv_sem=self.recv_sem.at[slot],
            device_id=dev, device_id_type=MESH).start()

    def plane_send(self, src, dst, g, rows, stage):
        mine = pl.ds(pl.multiple_of(self.me * rows, rows), rows)

        for t, dev in self.others:
            theirs = pl.ds(pl.multiple_of(t * rows, rows), rows)
            self.start(src.at[g, theirs], dst.at[g, mine], stage * GROUPS + g, dev)
        dst[g, mine, :] = src[g, mine, :]

    def plane_wait(self, dst, g, rows, stage, sem=None):
        part = dst.at[g, pl.ds(0, 31 * rows)]
        pltpu.make_async_copy(part, part, (self.recv_sem if sem is None else sem).at[stage * GROUPS + g]).wait()

    def axis_send(self, src_of, dst, axis, n, slot):
        def one(i, c):
            t, dev = self.axis_device(axis, n, i)
            self.start(src_of(t), dst.at[getattr(self, axis)], slot, dev)
            return c

        lax.fori_loop(0, n - 1, one, 0)

    def axis_wait(self, dst, n, slot, sem=None):
        part = dst.at[pl.ds(0, n - 1)]
        pltpu.make_async_copy(part, part, (self.recv_sem if sem is None else sem).at[slot]).wait()


def half_sums(row, low):
    a = jnp.sum(jnp.where(low, row, 0.0), axis=-1, keepdims=True)
    b = jnp.sum(jnp.where(low, 0.0, row), axis=-1, keepdims=True)
    return jnp.where(low, a, b)


def lane_low(shape):
    return lax.broadcasted_iota(jnp.int32, shape, len(shape) - 1) < HALF_LANES


def total(v):
    return jnp.sum(v.reshape(512, LANES), axis=0, keepdims=True)


def dft_stage(x_ref, g, m_ref, d_ref, st_ref):
    low = lane_low((1, LANES))
    v_all = x_ref[g].reshape(8, 4, 2, 16, LANES)
    cols = []
    for j in range(2):
        v = v_all[:, :, j]
        if st_ref is not None:
            mean = half_sums(total(v), low) * (1.0 / 32768.0)
            v = v - mean.reshape(1, 1, 1, LANES)
            var = half_sums(total(v * v), low) * (1.0 / 32768.0)
            inv = lax.rsqrt(var + NORM_EPS)
            v = v * inv.reshape(1, 1, 1, LANES)
            st_ref[g, j:j + 1, :] = mean
            st_ref[g, j + 4:j + 5, :] = inv
        cols.append(jnp.concatenate([v[:, w].reshape(LANES, LANES) for w in range(4)], axis=1))
    out = dot(m_ref[...], jnp.concatenate(cols, axis=0), NT)
    for half in range(2):
        for part in range(2):
            r0 = (half * 2 + part) * HALF_LANES
            for j in range(2):
                d_ref[g, pl.ds(part * 4 + j * 2 + half, HALF_LANES, stride=8), :] = out[r0:r0 + HALF_LANES, j * LANES:(j + 1) * LANES]


def idft_rows(z_ref, g, j, m_ref):
    parts = [z_ref[g, pl.ds(part * 4 + j * 2 + half, HALF_LANES, stride=8), :] for half in range(2) for part in range(2)]
    return dot(jnp.concatenate(parts, axis=0).T, m_ref[...], NN)


def join_grid(cols):
    per_j = [jnp.concatenate([c.reshape(8, 1, 16, LANES) for c in cols[j]], axis=1).reshape(8, 4, 1, 16, LANES) for j in range(2)]
    return jnp.concatenate(per_j, axis=2).reshape(1024, LANES)


def idft_stage(z_ref, g, m_ref, y_ref):
    cols = []
    for j in range(2):
        y = idft_rows(z_ref, g, j, m_ref)
        cols.append([y[:, w * LANES:(w + 1) * LANES] for w in range(4)])
    y_ref[g] = join_grid(cols)


def norm_back_stage(z_ref, g, m_ref, x_ref, st_ref, o_ref):
    low = lane_low((1, LANES))
    x_all = x_ref[g].reshape(8, 4, 2, 16, LANES)
    cols = []
    for j in range(2):
        y = idft_rows(z_ref, g, j, m_ref)
        mean, inv = st_ref[g, j:j + 1, :], st_ref[g, j + 4:j + 5, :]
        xs, ys, s0, s1 = [], [], 0.0, 0.0
        for w in range(4):
            yw = y[:, w * LANES:(w + 1) * LANES]
            xw = (x_all[:, w, j].reshape(LANES, LANES) - mean) * inv
            s0 = s0 + jnp.sum(yw, axis=0, keepdims=True)
            s1 = s1 + jnp.sum(yw * xw, axis=0, keepdims=True)
            xs.append(xw)
            ys.append(yw)
        s0 = half_sums(s0, low) * (1.0 / 32768.0)
        s1 = half_sums(s1, low) * (1.0 / 32768.0)
        cols.append([inv * (ys[w] - s0 - xs[w] * s1) for w in range(4)])
    o_ref[g] = join_grid(cols)


def swap_signed(t, top_sign):
    sub = lax.broadcasted_iota(jnp.int32, (8, LANES), 0)
    return jnp.where(sub < 4, top_sign, -top_sign) * pltpu.roll(t, 4, 0)


def to_degrees(x_ref, g, tab_ref):
    x = x_ref[g].reshape(CHANS, 2, 8, LANES)
    x = jnp.concatenate([x[:, 0].reshape(ROWS, LANES), x[:, 1].reshape(ROWS, LANES)], axis=1)
    return dot(x, tab_ref[...], NN)


def from_degrees(b, tab_ref, o_ref, g):
    y = dot(b, tab_ref[...], NT)
    y = jnp.concatenate([y[:, :LANES].reshape(CHANS, 1, 8, LANES), y[:, LANES:].reshape(CHANS, 1, 8, LANES)], axis=1)
    o_ref[g] = y.reshape(512, LANES)


def mix(src_ref, g, k_ref, dst_ref, adjoint):
    sign = 1.0 if adjoint else -1.0

    def body(c, acc):
        a = src_ref[g, pl.ds(pl.multiple_of(c * 8, 8), 8), :]
        s = swap_signed(a, sign)
        new = []
        for o in range(CHANS):
            if adjoint:
                kr, ki = k_ref[0, o, pl.ds(c, 1), :], k_ref[1, o, pl.ds(c, 1), :]
            else:
                kr, ki = k_ref[0, c, o:o + 1, :], k_ref[1, c, o:o + 1, :]
            new.append(acc[o] + (a * kr + s * ki))
        return tuple(new)

    acc = lax.fori_loop(0, CHANS, body, tuple(jnp.zeros((8, LANES), F32) for _ in range(CHANS)))
    for o in range(CHANS):
        dst_ref[o * 8:(o + 1) * 8, :] = acc[o]


def row_sums(v):
    sub = lax.broadcasted_iota(jnp.int32, (8, LANES), 0)
    low = sub < 4
    u = [jnp.where(low, v[j], v[j + 4]) + pltpu.roll(jnp.where(low, v[j + 4], v[j]), 4, 0) for j in range(4)]
    for step, n in ((2, 2), (1, 1)):
        first = lax.rem(sub // step, 2) == 0
        u = [jnp.where(first, u[j] + pltpu.roll(u[j], 8 - step, 0), u[j + n] + pltpu.roll(u[j + n], step, 0)) for j in range(n)]
    return u[0]


def kernel_grad(a_ref, d_ref, s_ref, gk_ref):
    def turn(o, carry):
        at = pl.ds(pl.multiple_of(o * 8, 8), 8)
        for g in range(GROUPS):
            s_ref[g, at, :] = swap_signed(d_ref[g, at, :], 1.0)
        return carry

    lax.fori_loop(0, CHANS, turn, 0)

    def rows(c, carry):
        at = pl.ds(pl.multiple_of(c * 8, 8), 8)
        a = [a_ref[g, at, :] for g in range(GROUPS)]
        for blk in range(4):
            for q, ref in ((0, d_ref), (1, s_ref)):
                prods = []
                for o in range(blk * 8, blk * 8 + 8):
                    prods.append(sum(a[g] * ref[g, o * 8:(o + 1) * 8, :] for g in range(GROUPS)))
                gk_ref[q, pl.ds(pl.multiple_of(c * CHANS + blk * 8, 8), 8), :] = row_sums(prods)
        return carry

    lax.fori_loop(0, CHANS, rows, 0)


def mlp_stage(y_ref, x_ref, t_ref, g, q, w1, w2, w1t, w2t, dy_ref, do_ref, sm_ref):
    for j in range(2):
        def take(ref):
            return jnp.concatenate([ref[g, pl.ds(j * 16 + r, CHANS, stride=CHANS), :] for r in range(16)], axis=1)

        y = take(y_ref)
        y_bf = y.astype(BF16)
        hid = dot(w1t, y_bf, NN, None)
        th = jnp.tanh(GELU_C * (hid + GELU_A * (hid * hid * hid)))
        cdf = 0.5 * (1.0 + th)
        act = (hid * cdf).astype(BF16)
        dgelu = cdf + (0.5 * hid * (1.0 - th * th)) * (GELU_C * (1.0 + (3.0 * GELU_A) * (hid * hid)))
        res = take(x_ref) + y + dot(w2t, act, NN, None) - take(t_ref)
        d_out = q * res
        sq = jnp.sum(d_out * res, axis=0, keepdims=True)
        sm_ref[CHANS:33, :] += sum(sq[:, r * LANES:(r + 1) * LANES] for r in range(16))
        d_bf = d_out.astype(BF16)
        g2 = dot(d_bf, act, NT, None)
        d_hid = (dot(w2, d_bf, NN, None) * dgelu).astype(BF16)
        g1 = dot(y_bf, d_hid, NT, None)
        sm_ref[0:CHANS, :] += jnp.concatenate([g1, g2], axis=1)
        d_y = d_out + dot(w1, d_hid, NN, None)
        for r in range(16):
            rows = pl.ds(j * 16 + r, CHANS, stride=CHANS)
            do_ref[g, rows, :] = d_out[:, r * LANES:(r + 1) * LANES]
            dy_ref[g, rows, :] = d_y[:, r * LANES:(r + 1) * LANES]


def pack_stage(x_ref, g, o_ref):
    parts = [jnp.concatenate([x_ref[g * 2 + j], x_ref[g * 2 + j + 6]], axis=-1) for j in range(2)]
    o_ref[g] = jnp.concatenate(parts, axis=1).reshape(1024, LANES)


BIG, HALF, SMALL = CHANS, 16, 40
EXTRA = 8 * GROUPS
(TAB, SM_A, SM_B, SM_C, GK_A, GK_B, GK_C) = range(EXTRA, EXTRA + 7)


def block_kernel(x_hbm, t_hbm, q_ref, w1_ref, w2t_ref, lp_ref, lq_ref, k_hbm, gf_hbm, gi_hbm,
                 out_hbm, gs_ref, smo_ref,
                 x_ref, t_ref, kw_ref, k_ref, gf_ref, gi_ref, q_row, tab,
                 s1, r1, s2, r2, s3, r3, s4, r4, s5, r5, s6, r6, s7, r7, s8, r8, tg, do,
                 st, acc_a, acc_d, acc_s, mixed, tabs, tp, tq, gk, gkt, gr1, gp, gr2, go, sm, sma, smb, smc, sb, sc,
                 send_sem, recv_sem, load_sem):
    links = Links(send_sem, recv_sem)
    low = lane_low((LANES, LANES))

    def load(src, dst, g, half):
        at = pl.ds(g * 2 + half * 6, 2)
        return pltpu.make_async_copy(src.at[at], dst.at[at], load_sem.at[(src is t_hbm) * 6 + g * 2 + half])

    for src, dst in ((x_hbm, x_ref), (t_hbm, t_ref)):
        for g in range(GROUPS):
            load(src, dst, g, 0).start()
            load(src, dst, g, 1).start()
        if src is x_hbm:
            tables = [pltpu.make_async_copy(a, b, load_sem.at[12 + i]) for i, (a, b) in enumerate(((gf_hbm, gf_ref), (k_hbm, kw_ref), (gi_hbm, gi_ref)))]
            for copy in tables:
                copy.start()
    links.greet()

    def groups(fn):
        def one(g, c):
            fn(g)
            return c

        lax.fori_loop(0, GROUPS, one, 0)

    def first(g):
        load(x_hbm, x_ref, g, 0).wait()
        load(x_hbm, x_ref, g, 1).wait()
        pack_stage(x_ref, g, s1)
        links.plane_send(s1, r1, g, BIG, 0)

    groups(first)
    for q, ref in ((0, lp_ref), (1, lq_ref)):
        for i in range(8):
            tab[i, q * 16:(q + 1) * 16, :] = jnp.concatenate([ref[2 * i], ref[2 * i + 1]], axis=1)
    links.axis_send(lambda t: tab.at[t], tabs, "h", 8, TAB)
    tabs[links.h] = tab[links.h]
    for r in range(16):
        q_row[:, r * LANES:(r + 1) * LANES] = jnp.full((1, LANES), q_ref[r], F32)
    for copy in tables:
        copy.wait()

    def widen(c, carry):
        for part in range(2):
            k_ref[part, c] = jnp.concatenate([kw_ref[part, c], kw_ref[part, c]], axis=1)
        return carry

    lax.fori_loop(0, CHANS, widen, 0)

    def take_target(g):
        load(t_hbm, t_ref, g, 0).wait()
        load(t_hbm, t_ref, g, 1).wait()
        pack_stage(t_ref, g, tg)

    groups(take_target)
    sm[...] = jnp.zeros((SMALL, LANES), F32)
    links.axis_wait(tabs, 8, TAB)
    for q, ref in ((0, tp), (1, tq)):
        rows = tabs[:, q * 16:(q + 1) * 16, :].reshape(LANES, LANES)
        ref[0:LANES, :] = jnp.where(low, rows, 0.0)
        ref[LANES:ROWS, :] = jnp.where(low, 0.0, rows)

    def second(g):
        links.plane_wait(r1, g, BIG, 0)
        dft_stage(r1, g, gf_ref, s2, st)
        links.plane_send(s2, r2, g, HALF, 1)

    def third(g):
        links.plane_wait(r2, g, HALF, 1)
        acc_a[g] = to_degrees(r2, g, tp)
        mix(acc_a, g, k_ref, mixed, False)
        from_degrees(mixed[...], tq, s3, g)
        links.plane_send(s3, r3, g, HALF, 2)

    def fourth(g):
        links.plane_wait(r3, g, HALF, 2)
        idft_stage(r3, g, gi_ref, s4)
        links.plane_send(s4, r4, g, BIG, 3)

    w1, w2t = w1_ref[...], w2t_ref[...]
    w1t, w2 = w1.astype(F32).T.astype(BF16), w2t.astype(F32).T.astype(BF16)

    def fifth(g):
        links.plane_wait(r4, g, BIG, 3)
        mlp_stage(r4, s1, tg, g, q_row[...], w1, w2, w1t, w2t, s5, do, sm)
        links.plane_send(s5, r5, g, BIG, 4)

    def sixth(g):
        links.plane_wait(r5, g, BIG, 4)
        dft_stage(r5, g, gi_ref, s6, None)
        links.plane_send(s6, r6, g, HALF, 5)

    def seventh(g):
        links.plane_wait(r6, g, HALF, 5)
        acc_d[g] = to_degrees(r6, g, tq)
        mix(acc_d, g, k_ref, mixed, True)
        from_degrees(mixed[...], tp, s7, g)
        links.plane_send(s7, r7, g, HALF, 6)

    def eighth(g):
        links.plane_wait(r7, g, HALF, 6)
        norm_back_stage(r7, g, gf_ref, r1, st, s8)

    def ninth(g):
        links.plane_wait(r8, g, BIG, 7)
        do[g] = do[g] + r8[g]
        pltpu.make_async_copy(do.at[g], out_hbm.at[g], load_sem.at[15 + g]).start()

    for stage in (second, third, fourth, fifth):
        groups(stage)

    links.axis_send(lambda t: sm, sma, "dp", 8, SM_A)
    sma[links.dp] = sm[...]
    groups(sixth)
    links.axis_wait(sma, 8, SM_A)
    sb[...] = jnp.sum(sma[...], axis=0)
    links.axis_send(lambda t: sb, smb, "h", 8, SM_B)
    smb[links.h] = sb[...]
    groups(seventh)
    links.axis_wait(smb, 8, SM_B)
    sc[...] = jnp.sum(smb[...], axis=0)
    links.axis_send(lambda t: sc, smc, "w", 4, SM_C)
    smc[links.w] = sc[...]


    kernel_grad(acc_a, acc_d, acc_s, gk)

    def turn(n, c):
        for q in range(2):
            t = gk[q, pl.ds(pl.multiple_of(n * LANES, LANES), LANES), :].T
            i = q * 8 + n
            gkt[i // 2, pl.ds(pl.multiple_of(lax.rem(i, 2) * HALF_LANES, HALF_LANES), HALF_LANES), :] = t[0:HALF_LANES] + t[HALF_LANES:LANES]
        return c

    lax.fori_loop(0, 8, turn, 0)
    links.axis_send(lambda t: gkt.at[t], gr1, "dp", 8, GK_A)
    gr1[links.dp] = gkt[links.dp]
    for g in range(2):
        eighth(g)
        links.plane_send(s8, r8, g, BIG, 7)
    eighth(2)
    links.axis_wait(gr1, 8, GK_A)
    part = jnp.sum(gr1[...], axis=0)
    for n in range(2):
        gp[:, n * 8:(n + 1) * 8, :] = part[n * HALF_LANES:(n + 1) * HALF_LANES].reshape(8, 8, LANES)

    for t, dev in links.others:
        links.start(gp.at[t // 4], gr2.at[links.me], GK_B, dev)
    links.plane_send(s8, r8, 2, BIG, 7)
    gr2[links.me] = gp[links.h]
    ninth(0)
    links.axis_wait(gr2, CHANS, GK_B)
    go[...] = jnp.sum(gr2[...], axis=0)
    links.axis_send(lambda t: go, gs_ref, "dp", 8, GK_C)
    gs_ref[links.dp] = go[...]
    links.axis_wait(smc, 4, SM_C)
    sums = jnp.sum(smc[...], axis=0)
    smo_ref[0:CHANS, :] = sums[0:CHANS]
    smo_ref[CHANS:40, :] = sums[CHANS:40] * (1.0 / 100663296.0)
    ninth(1)
    ninth(2)
    links.axis_wait(gs_ref, 8, GK_C)
    for g in range(GROUPS):
        pltpu.make_async_copy(do.at[g], out_hbm.at[g], load_sem.at[15 + g]).wait()

    for stage, (buf, rows) in enumerate(((s1, BIG), (s2, HALF), (s3, HALF), (s4, BIG), (s5, BIG), (s6, HALF), (s7, HALF), (s8, BIG))):
        groups(lambda g, buf=buf, rows=rows, stage=stage: links.plane_wait(buf, g, rows, stage, send_sem))
    for buf, n, slot in ((tabs, 8, TAB), (sma, 8, SM_A), (smb, 8, SM_B), (smc, 4, SM_C), (gr1, 8, GK_A), (gr2, CHANS, GK_B), (gs_ref, 8, GK_C)):
        links.axis_wait(buf, n, slot, send_sem)


def run_block(*args):
    big, half = pltpu.VMEM((GROUPS, 1024, LANES), F32), pltpu.VMEM((GROUPS, 512, LANES), F32)
    stages = [big, big, half, half, half, half, big, big, big, big, half, half, half, half, big, big, big, big]
    vm = lambda *s: pltpu.VMEM(s, F32)
    fields = [vm(12, CHANS, 16, HALF_LANES), vm(12, CHANS, 16, HALF_LANES), vm(2, CHANS, CHANS, HALF_LANES), vm(2, CHANS, CHANS, LANES), vm(ROWS, 512), vm(ROWS, 512), vm(1, 2048), vm(8, CHANS, LANES)]
    scratch = fields + stages + [
        vm(GROUPS, 8, LANES), vm(GROUPS, ROWS, LANES), vm(GROUPS, ROWS, LANES), vm(GROUPS, ROWS, LANES), vm(ROWS, LANES),
        vm(8, CHANS, LANES), vm(ROWS, LANES), vm(ROWS, LANES),
        vm(2, 1024, LANES), vm(8, LANES, LANES), vm(8, LANES, LANES), vm(8, 16, LANES), vm(CHANS, 16, LANES), vm(16, LANES),
        vm(SMALL, LANES), vm(8, SMALL, LANES), vm(8, SMALL, LANES), vm(4, SMALL, LANES), vm(SMALL, LANES), vm(SMALL, LANES),
        pltpu.SemaphoreType.DMA((EXTRA + 7,)), pltpu.SemaphoreType.DMA((EXTRA + 7,)), pltpu.SemaphoreType.DMA((18,)),
    ]
    space, hbm = pl.BlockSpec(memory_space=pltpu.VMEM), pl.BlockSpec(memory_space=pl.ANY)
    return pl.pallas_call(
        block_kernel,
        out_shape=[
            jax.ShapeDtypeStruct((GROUPS, 1024, LANES), F32),
            jax.ShapeDtypeStruct((8, 16, LANES), F32),
            jax.ShapeDtypeStruct((SMALL, LANES), F32),
        ],
        in_specs=[hbm, hbm, pl.BlockSpec(memory_space=pltpu.SMEM), space, space, space, space, hbm, hbm, hbm],
        out_specs=[hbm, space, space],
        scratch_shapes=scratch,
        compiler_params=pltpu.CompilerParams(collective_id=0, has_side_effects=True, vmem_limit_bytes=62 * 1024 * 1024),
        name="block",
    )(*args)


def unpack_kernel(v_ref, sm_ref, o_ref, g1_ref, g2_ref, loss_ref):
    for j in range(2):
        v = v_ref[0, :, j * 16:(j + 1) * 16, :]
        o_ref[0, j] = v[:, :, :HALF_LANES]
        o_ref[1, j] = v[:, :, HALF_LANES:]

    @pl.when(pl.program_id(0) == 0)
    def _():
        g1_ref[...] = sm_ref[0:CHANS, 0:HALF_LANES]
        g2_ref[...] = sm_ref[0:CHANS, HALF_LANES:LANES]
        loss_ref[...] = jnp.sum(sm_ref[CHANS:33, :], axis=1, keepdims=True)


def unpack(v, sm):
    whole = lambda *shape: pl.BlockSpec(shape, lambda g: (0, 0))
    out, g1, g2, loss = pl.pallas_call(
        unpack_kernel,
        grid=(GROUPS,),
        in_specs=[pl.BlockSpec((1, CHANS, CHANS, LANES), lambda g: (g, 0, 0, 0)), whole(SMALL, LANES)],
        out_specs=[pl.BlockSpec((2, 2, CHANS, 16, HALF_LANES), lambda g: (0, g, 0, 0, 0)), whole(CHANS, HALF_LANES), whole(CHANS, HALF_LANES), whole(1, 1)],
        out_shape=[jax.ShapeDtypeStruct((2, 6, CHANS, 16, HALF_LANES), F32), jax.ShapeDtypeStruct((CHANS, HALF_LANES), F32),
                   jax.ShapeDtypeStruct((CHANS, HALF_LANES), F32), jax.ShapeDtypeStruct((1, 1), F32)],
        name="unpack",
    )(v.reshape(GROUPS, CHANS, CHANS, LANES), sm)
    return out.reshape(12, CHANS, 16, HALF_LANES), g1, g2.T, loss[0, 0]


def solution(mesh):
    w_size, h_size, dp_size = mesh.shape["w"], mesh.shape["h"], mesh.shape["dp"]
    fwd_np, inv_np = dft_tables(ROWS, HALF_LANES, w_size, h_size)

    def local_step(field, target, lat_weight, leg_fwd, leg_inv, spec_w, w_in, w_out):
        gf, gi = jnp.asarray(fwd_np), jnp.asarray(inv_np)
        packed, gs, sm = run_block(
            field, target, lat_weight, w_in, w_out.T, leg_fwd.transpose(0, 2, 1), leg_inv.transpose(0, 2, 1),
            spec_w.transpose(0, 2, 3, 1), gf, gi)
        d_field, grad_w_in, grad_w_out, loss = unpack(packed, sm)
        grad_spec = gs.reshape(2, 4, 2, 8, 4, CHANS).transpose(0, 3, 1, 2, 4, 5).reshape(2, 8, CHANS, CHANS)
        return loss, d_field, grad_spec, grad_w_in, grad_w_out

    grid_spec = P("dp", None, "h", "w")
    table_spec = P("w", None, "h")
    kernel_out = P(None, "h", None, None)
    return jax.shard_map(local_step, mesh=mesh, in_specs=(grid_spec, grid_spec, P("h"), table_spec, table_spec, P(), P(), P()), out_specs=(P(), grid_spec, kernel_out, P(), P()), check_vma=False)
```

```python
import functools
import numpy as np
import jax
import jax.numpy as jnp
from jax import lax
from jax.experimental import pallas as pl
from jax.experimental.pallas import tpu as pltpu
from jax.sharding import PartitionSpec as P

NORM_EPS = 1e-5
HI = lax.Precision.HIGHEST
GELU_C = 0.7978845608028654
GELU_A = 0.044715
NT = (((1,), (1,)), ((), ()))
NN = (((1,), (0,)), ((), ()))
F32 = jnp.float32
LANES, HALF_LANES, CHANS, ROWS = 128, 64, 32, 256
BF16 = jnp.bfloat16


def dot(a, b, dims, precision=HI):
    return lax.dot_general(a, b, dims, precision=precision, preferred_element_type=F32)


def dft_tables(nlon, modes, w_size, h_size):
    per = modes // (w_size * h_size)
    order = [w * (modes // w_size) + h * per + j for h in range(h_size) for w in range(w_size) for j in range(per)]
    m = np.array(order)[:, None]
    n = np.arange(nlon)[None, :]
    ang = 2.0 * np.pi * ((m * n) % nlon) / nlon
    fwd = np.concatenate([np.cos(ang), -np.sin(ang)]) / np.sqrt(nlon)
    mult = np.where(m == 0, 1.0, 2.0)
    inv = np.concatenate([mult * np.cos(ang), -mult * np.sin(ang)]) / np.sqrt(nlon)
    lon = nlon // w_size

    def spread(t):
        out = np.zeros((2, 2 * modes, w_size, 2, lon))
        for half in range(2):
            out[half, :, :, half, :] = t.reshape(2 * modes, w_size, lon)
        return out.reshape(4 * modes, 2 * nlon).astype(np.float32)

    return spread(fwd), spread(inv)

GROUPS = 3
MESH = pl.DeviceIdType.MESH


CHIPS = [int(d, 16) for d in "5af49e38d27c16b"]


class Links:
    def __init__(self, send_sem, recv_sem):
        self.h, self.w, self.dp = lax.axis_index("h"), lax.axis_index("w"), lax.axis_index("dp")
        self.me = self.h * 4 + self.w
        self.send_sem, self.recv_sem = send_sem, recv_sem
        self.others = [self.plane_device(i) for i in range(31)]

    def plane_device(self, i):
        chip, core = (CHIPS[i], 0) if i < 15 else ((0, *CHIPS)[i - 15], 1)
        x = lax.rem(self.h // 2 + chip % 4, 4)
        w = lax.rem(self.w + chip // 4, 4)
        h = x * 2 + lax.rem(self.h + core, 2)
        return h * 4 + w, {"h": h, "w": w}

    def axis_device(self, axis, n, i):
        t = lax.rem(getattr(self, axis) + 1 + i, n)
        return t, {axis: t}

    def greet(self):
        bar = pltpu.get_barrier_semaphore()

        def depth(i, c):
            pl.semaphore_signal(bar, inc=1, device_id=self.axis_device("dp", 8, i)[1], device_id_type=MESH)
            return c

        for _, dev in self.others:
            pl.semaphore_signal(bar, inc=1, device_id=dev, device_id_type=MESH)
        lax.fori_loop(0, 7, depth, 0)
        pl.semaphore_wait(bar, 38)

    def start(self, src, dst, slot, dev):
        pltpu.make_async_remote_copy(
            src_ref=src, dst_ref=dst, send_sem=self.send_sem.at[slot], recv_sem=self.recv_sem.at[slot],
            device_id=dev, device_id_type=MESH).start()

    def plane_send(self, src, dst, g, rows, stage):
        mine = pl.ds(pl.multiple_of(self.me * rows, rows), rows)

        for t, dev in self.others:
            theirs = pl.ds(pl.multiple_of(t * rows, rows), rows)
            self.start(src.at[g, theirs], dst.at[g, mine], stage * GROUPS + g, dev)
        dst[g, mine, :] = src[g, mine, :]

    def plane_wait(self, dst, g, rows, stage, sem=None):
        part = dst.at[g, pl.ds(0, 31 * rows)]
        pltpu.make_async_copy(part, part, (self.recv_sem if sem is None else sem).at[stage * GROUPS + g]).wait()

    def axis_send(self, src_of, dst, axis, n, slot):
        def one(i, c):
            t, dev = self.axis_device(axis, n, i)
            self.start(src_of(t), dst.at[getattr(self, axis)], slot, dev)
            return c

        lax.fori_loop(0, n - 1, one, 0)

    def axis_wait(self, dst, n, slot, sem=None):
        part = dst.at[pl.ds(0, n - 1)]
        pltpu.make_async_copy(part, part, (self.recv_sem if sem is None else sem).at[slot]).wait()


def half_sums(row, low):
    a = jnp.sum(jnp.where(low, row, 0.0), axis=-1, keepdims=True)
    b = jnp.sum(jnp.where(low, 0.0, row), axis=-1, keepdims=True)
    return jnp.where(low, a, b)


def lane_low(shape):
    return lax.broadcasted_iota(jnp.int32, shape, len(shape) - 1) < HALF_LANES


def total(v):
    return jnp.sum(v.reshape(512, LANES), axis=0, keepdims=True)


def dft_stage(x_ref, g, m_ref, d_ref, st_ref):
    low = lane_low((1, LANES))
    v_all = x_ref[g].reshape(8, 4, 2, 16, LANES)
    cols = []
    for j in range(2):
        v = v_all[:, :, j]
        if st_ref is not None:
            mean = half_sums(total(v), low) * (1.0 / 32768.0)
            v = v - mean.reshape(1, 1, 1, LANES)
            var = half_sums(total(v * v), low) * (1.0 / 32768.0)
            inv = lax.rsqrt(var + NORM_EPS)
            v = v * inv.reshape(1, 1, 1, LANES)
            st_ref[g, j:j + 1, :] = mean
            st_ref[g, j + 4:j + 5, :] = inv
        cols.append(jnp.concatenate([v[:, w].reshape(LANES, LANES) for w in range(4)], axis=1))
    out = dot(m_ref[...], jnp.concatenate(cols, axis=0), NT)
    for half in range(2):
        for part in range(2):
            r0 = (half * 2 + part) * HALF_LANES
            for j in range(2):
                d_ref[g, pl.ds(part * 4 + j * 2 + half, HALF_LANES, stride=8), :] = out[r0:r0 + HALF_LANES, j * LANES:(j + 1) * LANES]


def idft_rows(z_ref, g, j, m_ref):
    parts = [z_ref[g, pl.ds(part * 4 + j * 2 + half, HALF_LANES, stride=8), :] for half in range(2) for part in range(2)]
    return dot(jnp.concatenate(parts, axis=0).T, m_ref[...], NN)


def join_grid(cols):
    per_j = [jnp.concatenate([c.reshape(8, 1, 16, LANES) for c in cols[j]], axis=1).reshape(8, 4, 1, 16, LANES) for j in range(2)]
    return jnp.concatenate(per_j, axis=2).reshape(1024, LANES)


def idft_stage(z_ref, g, m_ref, y_ref):
    cols = []
    for j in range(2):
        y = idft_rows(z_ref, g, j, m_ref)
        cols.append([y[:, w * LANES:(w + 1) * LANES] for w in range(4)])
    y_ref[g] = join_grid(cols)


def norm_back_stage(z_ref, g, m_ref, x_ref, st_ref, o_ref):
    low = lane_low((1, LANES))
    x_all = x_ref[g].reshape(8, 4, 2, 16, LANES)
    cols = []
    for j in range(2):
        y = idft_rows(z_ref, g, j, m_ref)
        mean, inv = st_ref[g, j:j + 1, :], st_ref[g, j + 4:j + 5, :]
        xs, ys, s0, s1 = [], [], 0.0, 0.0
        for w in range(4):
            yw = y[:, w * LANES:(w + 1) * LANES]
            xw = (x_all[:, w, j].reshape(LANES, LANES) - mean) * inv
            s0 = s0 + jnp.sum(yw, axis=0, keepdims=True)
            s1 = s1 + jnp.sum(yw * xw, axis=0, keepdims=True)
            xs.append(xw)
            ys.append(yw)
        s0 = half_sums(s0, low) * (1.0 / 32768.0)
        s1 = half_sums(s1, low) * (1.0 / 32768.0)
        cols.append([inv * (ys[w] - s0 - xs[w] * s1) for w in range(4)])
    o_ref[g] = join_grid(cols)


def swap_signed(t, top_sign):
    sub = lax.broadcasted_iota(jnp.int32, (8, LANES), 0)
    return jnp.where(sub < 4, top_sign, -top_sign) * pltpu.roll(t, 4, 0)


def to_degrees(x_ref, g, tab_ref):
    x = x_ref[g].reshape(CHANS, 2, 8, LANES)
    x = jnp.concatenate([x[:, 0].reshape(ROWS, LANES), x[:, 1].reshape(ROWS, LANES)], axis=1)
    return dot(x, tab_ref[...], NN)


def from_degrees(b, tab_ref, o_ref, g):
    y = dot(b, tab_ref[...], NT)
    y = jnp.concatenate([y[:, :LANES].reshape(CHANS, 1, 8, LANES), y[:, LANES:].reshape(CHANS, 1, 8, LANES)], axis=1)
    o_ref[g] = y.reshape(512, LANES)


def mix(src_ref, g, k_ref, dst_ref, adjoint):
    sign = 1.0 if adjoint else -1.0

    def body(c, acc):
        a = src_ref[g, pl.ds(pl.multiple_of(c * 8, 8), 8), :]
        s = swap_signed(a, sign)
        new = []
        for o in range(CHANS):
            if adjoint:
                kr, ki = k_ref[0, o, pl.ds(c, 1), :], k_ref[1, o, pl.ds(c, 1), :]
            else:
                kr, ki = k_ref[0, c, o:o + 1, :], k_ref[1, c, o:o + 1, :]
            new.append(acc[o] + (a * kr + s * ki))
        return tuple(new)

    acc = lax.fori_loop(0, CHANS, body, tuple(jnp.zeros((8, LANES), F32) for _ in range(CHANS)))
    for o in range(CHANS):
        dst_ref[o * 8:(o + 1) * 8, :] = acc[o]


def row_sums(v):
    sub = lax.broadcasted_iota(jnp.int32, (8, LANES), 0)
    low = sub < 4
    u = [jnp.where(low, v[j], v[j + 4]) + pltpu.roll(jnp.where(low, v[j + 4], v[j]), 4, 0) for j in range(4)]
    for step, n in ((2, 2), (1, 1)):
        first = lax.rem(sub // step, 2) == 0
        u = [jnp.where(first, u[j] + pltpu.roll(u[j], 8 - step, 0), u[j + n] + pltpu.roll(u[j + n], step, 0)) for j in range(n)]
    return u[0]


def kernel_grad(a_ref, d_ref, s_ref, gk_ref):
    def turn(o, carry):
        at = pl.ds(pl.multiple_of(o * 8, 8), 8)
        for g in range(GROUPS):
            s_ref[g, at, :] = swap_signed(d_ref[g, at, :], 1.0)
        return carry

    lax.fori_loop(0, CHANS, turn, 0)

    def rows(c, carry):
        at = pl.ds(pl.multiple_of(c * 8, 8), 8)
        a = [a_ref[g, at, :] for g in range(GROUPS)]
        for blk in range(4):
            for q, ref in ((0, d_ref), (1, s_ref)):
                prods = []
                for o in range(blk * 8, blk * 8 + 8):
                    prods.append(sum(a[g] * ref[g, o * 8:(o + 1) * 8, :] for g in range(GROUPS)))
                gk_ref[q, pl.ds(pl.multiple_of(c * CHANS + blk * 8, 8), 8), :] = row_sums(prods)
        return carry

    lax.fori_loop(0, CHANS, rows, 0)


def mlp_stage(y_ref, x_ref, t_ref, g, q, w1, w2, w1t, w2t, dy_ref, do_ref, sm_ref):
    for j in range(2):
        def take(ref):
            return jnp.concatenate([ref[g, pl.ds(j * 16 + r, CHANS, stride=CHANS), :] for r in range(16)], axis=1)

        y = take(y_ref)
        y_bf = y.astype(BF16)
        hid = dot(w1t, y_bf, NN, None)
        th = jnp.tanh(GELU_C * (hid + GELU_A * (hid * hid * hid)))
        cdf = 0.5 * (1.0 + th)
        act = (hid * cdf).astype(BF16)
        dgelu = cdf + (0.5 * hid * (1.0 - th * th)) * (GELU_C * (1.0 + (3.0 * GELU_A) * (hid * hid)))
        res = take(x_ref) + y + dot(w2t, act, NN, None) - take(t_ref)
        d_out = q * res
        sq = jnp.sum(d_out * res, axis=0, keepdims=True)
        sm_ref[CHANS:33, :] += sum(sq[:, r * LANES:(r + 1) * LANES] for r in range(16))
        d_bf = d_out.astype(BF16)
        g2 = dot(d_bf, act, NT, None)
        d_hid = (dot(w2, d_bf, NN, None) * dgelu).astype(BF16)
        g1 = dot(y_bf, d_hid, NT, None)
        sm_ref[0:CHANS, :] += jnp.concatenate([g1, g2], axis=1)
        d_y = d_out + dot(w1, d_hid, NN, None)
        for r in range(16):
            rows = pl.ds(j * 16 + r, CHANS, stride=CHANS)
            do_ref[g, rows, :] = d_out[:, r * LANES:(r + 1) * LANES]
            dy_ref[g, rows, :] = d_y[:, r * LANES:(r + 1) * LANES]


def pack_stage(x_ref, g, o_ref):
    parts = [jnp.concatenate([x_ref[g * 2 + j], x_ref[g * 2 + j + 6]], axis=-1) for j in range(2)]
    o_ref[g] = jnp.concatenate(parts, axis=1).reshape(1024, LANES)


BIG, HALF, SMALL = CHANS, 16, 40
EXTRA = 8 * GROUPS
(TAB, SM_A, SM_B, SM_C, GK_A, GK_B, GK_C) = range(EXTRA, EXTRA + 7)


def block_kernel(x_hbm, t_hbm, q_ref, w1_ref, w2t_ref, lp_ref, lq_ref, k_hbm, gf_hbm, gi_hbm,
                 out_hbm, gs_ref, smo_ref,
                 x_ref, t_ref, kw_ref, k_ref, gf_ref, gi_ref, q_row, tab,
                 s1, r1, s2, r2, s3, r3, s4, r4, s5, r5, s6, r6, s7, r7, s8, r8, tg, do,
                 st, acc_a, acc_d, acc_s, mixed, tabs, tp, tq, gk, gkt, gr1, gp, gr2, go, sm, sma, smb, smc, sb, sc,
                 send_sem, recv_sem, load_sem):
    links = Links(send_sem, recv_sem)
    low = lane_low((LANES, LANES))

    def load(src, dst, g, half):
        at = pl.ds(g * 2 + half * 6, 2)
        return pltpu.make_async_copy(src.at[at], dst.at[at], load_sem.at[(src is t_hbm) * 6 + g * 2 + half])

    for src, dst in ((x_hbm, x_ref), (t_hbm, t_ref)):
        for g in range(GROUPS):
            load(src, dst, g, 0).start()
            load(src, dst, g, 1).start()
        if src is x_hbm:
            tables = [pltpu.make_async_copy(a, b, load_sem.at[12 + i]) for i, (a, b) in enumerate(((gf_hbm, gf_ref), (k_hbm, kw_ref), (gi_hbm, gi_ref)))]
            for copy in tables:
                copy.start()
    links.greet()

    def groups(fn):
        def one(g, c):
            fn(g)
            return c

        lax.fori_loop(0, GROUPS, one, 0)

    def first(g):
        load(x_hbm, x_ref, g, 0).wait()
        load(x_hbm, x_ref, g, 1).wait()
        pack_stage(x_ref, g, s1)
        links.plane_send(s1, r1, g, BIG, 0)

    groups(first)
    for q, ref in ((0, lp_ref), (1, lq_ref)):
        for i in range(8):
            tab[i, q * 16:(q + 1) * 16, :] = jnp.concatenate([ref[2 * i], ref[2 * i + 1]], axis=1)
    links.axis_send(lambda t: tab.at[t], tabs, "h", 8, TAB)
    tabs[links.h] = tab[links.h]
    for r in range(16):
        q_row[:, r * LANES:(r + 1) * LANES] = jnp.full((1, LANES), q_ref[r], F32)
    for copy in tables:
        copy.wait()

    def widen(c, carry):
        for part in range(2):
            k_ref[part, c] = jnp.concatenate([kw_ref[part, c], kw_ref[part, c]], axis=1)
        return carry

    lax.fori_loop(0, CHANS, widen, 0)

    def take_target(g):
        load(t_hbm, t_ref, g, 0).wait()
        load(t_hbm, t_ref, g, 1).wait()
        pack_stage(t_ref, g, tg)

    groups(take_target)
    sm[...] = jnp.zeros((SMALL, LANES), F32)
    def second(g):
        links.plane_wait(r1, g, BIG, 0)
        dft_stage(r1, g, gf_ref, s2, st)
        links.plane_send(s2, r2, g, HALF, 1)

    def third(g):
        links.plane_wait(r2, g, HALF, 1)
        acc_a[g] = to_degrees(r2, g, tp)
        mix(acc_a, g, k_ref, mixed, False)
        from_degrees(mixed[...], tq, s3, g)
        links.plane_send(s3, r3, g, HALF, 2)

    def fourth(g):
        links.plane_wait(r3, g, HALF, 2)
        idft_stage(r3, g, gi_ref, s4)
        links.plane_send(s4, r4, g, BIG, 3)

    w1, w2t = w1_ref[...], w2t_ref[...]
    w1t, w2 = w1.astype(F32).T.astype(BF16), w2t.astype(F32).T.astype(BF16)

    def fifth(g):
        links.plane_wait(r4, g, BIG, 3)
        mlp_stage(r4, s1, tg, g, q_row[...], w1, w2, w1t, w2t, s5, do, sm)
        links.plane_send(s5, r5, g, BIG, 4)

    def sixth(g):
        links.plane_wait(r5, g, BIG, 4)
        dft_stage(r5, g, gi_ref, s6, None)
        links.plane_send(s6, r6, g, HALF, 5)

    def seventh(g):
        links.plane_wait(r6, g, HALF, 5)
        acc_d[g] = to_degrees(r6, g, tq)
        mix(acc_d, g, k_ref, mixed, True)
        from_degrees(mixed[...], tp, s7, g)
        links.plane_send(s7, r7, g, HALF, 6)

    def eighth(g):
        links.plane_wait(r7, g, HALF, 6)
        norm_back_stage(r7, g, gf_ref, r1, st, s8)

    def ninth(g):
        links.plane_wait(r8, g, BIG, 7)
        do[g] = do[g] + r8[g]
        pltpu.make_async_copy(do.at[g], out_hbm.at[g], load_sem.at[15 + g]).start()

    groups(second)
    links.axis_wait(tabs, 8, TAB)
    for q, ref in ((0, tp), (1, tq)):
        rows = tabs[:, q * 16:(q + 1) * 16, :].reshape(LANES, LANES)
        ref[0:LANES, :] = jnp.where(low, rows, 0.0)
        ref[LANES:ROWS, :] = jnp.where(low, 0.0, rows)
    for stage in (third, fourth, fifth):
        groups(stage)

    links.axis_send(lambda t: sm, sma, "dp", 8, SM_A)
    sma[links.dp] = sm[...]
    groups(sixth)
    links.axis_wait(sma, 8, SM_A)
    sb[...] = jnp.sum(sma[...], axis=0)
    links.axis_send(lambda t: sb, smb, "h", 8, SM_B)
    smb[links.h] = sb[...]
    groups(seventh)
    links.axis_wait(smb, 8, SM_B)
    sc[...] = jnp.sum(smb[...], axis=0)
    links.axis_send(lambda t: sc, smc, "w", 4, SM_C)
    smc[links.w] = sc[...]


    kernel_grad(acc_a, acc_d, acc_s, gk)

    def turn(n, c):
        for q in range(2):
            t = gk[q, pl.ds(pl.multiple_of(n * LANES, LANES), LANES), :].T
            i = q * 8 + n
            gkt[i // 2, pl.ds(pl.multiple_of(lax.rem(i, 2) * HALF_LANES, HALF_LANES), HALF_LANES), :] = t[0:HALF_LANES] + t[HALF_LANES:LANES]
        return c

    lax.fori_loop(0, 8, turn, 0)
    links.axis_send(lambda t: gkt.at[t], gr1, "dp", 8, GK_A)
    gr1[links.dp] = gkt[links.dp]
    for g in range(2):
        eighth(g)
        links.plane_send(s8, r8, g, BIG, 7)
    eighth(2)
    links.axis_wait(gr1, 8, GK_A)
    part = jnp.sum(gr1[...], axis=0)
    for n in range(2):
        gp[:, n * 8:(n + 1) * 8, :] = part[n * HALF_LANES:(n + 1) * HALF_LANES].reshape(8, 8, LANES)

    for t, dev in links.others:
        links.start(gp.at[t // 4], gr2.at[links.me], GK_B, dev)
    links.plane_send(s8, r8, 2, BIG, 7)
    gr2[links.me] = gp[links.h]
    ninth(0)
    links.axis_wait(gr2, CHANS, GK_B)
    go[...] = jnp.sum(gr2[...], axis=0)
    links.axis_send(lambda t: go, gs_ref, "dp", 8, GK_C)
    gs_ref[links.dp] = go[...]
    links.axis_wait(smc, 4, SM_C)
    sums = jnp.sum(smc[...], axis=0)
    smo_ref[0:CHANS, :] = sums[0:CHANS]
    smo_ref[CHANS:40, :] = sums[CHANS:40] * (1.0 / 100663296.0)
    ninth(1)
    ninth(2)
    links.axis_wait(gs_ref, 8, GK_C)
    for g in range(GROUPS):
        pltpu.make_async_copy(do.at[g], out_hbm.at[g], load_sem.at[15 + g]).wait()

    for stage, (buf, rows) in enumerate(((s1, BIG), (s2, HALF), (s3, HALF), (s4, BIG), (s5, BIG), (s6, HALF), (s7, HALF), (s8, BIG))):
        groups(lambda g, buf=buf, rows=rows, stage=stage: links.plane_wait(buf, g, rows, stage, send_sem))
    for buf, n, slot in ((tabs, 8, TAB), (sma, 8, SM_A), (smb, 8, SM_B), (smc, 4, SM_C), (gr1, 8, GK_A), (gr2, CHANS, GK_B), (gs_ref, 8, GK_C)):
        links.axis_wait(buf, n, slot, send_sem)


def run_block(*args):
    big, half = pltpu.VMEM((GROUPS, 1024, LANES), F32), pltpu.VMEM((GROUPS, 512, LANES), F32)
    stages = [big, big, half, half, half, half, big, big, big, big, half, half, half, half, big, big, big, big]
    vm = lambda *s: pltpu.VMEM(s, F32)
    fields = [vm(12, CHANS, 16, HALF_LANES), vm(12, CHANS, 16, HALF_LANES), vm(2, CHANS, CHANS, HALF_LANES), vm(2, CHANS, CHANS, LANES), vm(ROWS, 512), vm(ROWS, 512), vm(1, 2048), vm(8, CHANS, LANES)]
    scratch = fields + stages + [
        vm(GROUPS, 8, LANES), vm(GROUPS, ROWS, LANES), vm(GROUPS, ROWS, LANES), vm(GROUPS, ROWS, LANES), vm(ROWS, LANES),
        vm(8, CHANS, LANES), vm(ROWS, LANES), vm(ROWS, LANES),
        vm(2, 1024, LANES), vm(8, LANES, LANES), vm(8, LANES, LANES), vm(8, 16, LANES), vm(CHANS, 16, LANES), vm(16, LANES),
        vm(SMALL, LANES), vm(8, SMALL, LANES), vm(8, SMALL, LANES), vm(4, SMALL, LANES), vm(SMALL, LANES), vm(SMALL, LANES),
        pltpu.SemaphoreType.DMA((EXTRA + 7,)), pltpu.SemaphoreType.DMA((EXTRA + 7,)), pltpu.SemaphoreType.DMA((18,)),
    ]
    space, hbm = pl.BlockSpec(memory_space=pltpu.VMEM), pl.BlockSpec(memory_space=pl.ANY)
    return pl.pallas_call(
        block_kernel,
        out_shape=[
            jax.ShapeDtypeStruct((GROUPS, 1024, LANES), F32),
            jax.ShapeDtypeStruct((8, 16, LANES), F32),
            jax.ShapeDtypeStruct((SMALL, LANES), F32),
        ],
        in_specs=[hbm, hbm, pl.BlockSpec(memory_space=pltpu.SMEM), space, space, space, space, hbm, hbm, hbm],
        out_specs=[hbm, space, space],
        scratch_shapes=scratch,
        compiler_params=pltpu.CompilerParams(collective_id=0, has_side_effects=True, vmem_limit_bytes=62 * 1024 * 1024),
        name="block",
    )(*args)


def unpack_kernel(v_ref, sm_ref, o_ref, g1_ref, g2_ref, loss_ref):
    for j in range(2):
        v = v_ref[0, :, j * 16:(j + 1) * 16, :]
        o_ref[0, j] = v[:, :, :HALF_LANES]
        o_ref[1, j] = v[:, :, HALF_LANES:]

    @pl.when(pl.program_id(0) == 0)
    def _():
        g1_ref[...] = sm_ref[0:CHANS, 0:HALF_LANES]
        g2_ref[...] = sm_ref[0:CHANS, HALF_LANES:LANES]
        loss_ref[...] = jnp.sum(sm_ref[CHANS:33, :], axis=1, keepdims=True)


def unpack(v, sm):
    whole = lambda *shape: pl.BlockSpec(shape, lambda g: (0, 0))
    out, g1, g2, loss = pl.pallas_call(
        unpack_kernel,
        grid=(GROUPS,),
        in_specs=[pl.BlockSpec((1, CHANS, CHANS, LANES), lambda g: (g, 0, 0, 0)), whole(SMALL, LANES)],
        out_specs=[pl.BlockSpec((2, 2, CHANS, 16, HALF_LANES), lambda g: (0, g, 0, 0, 0)), whole(CHANS, HALF_LANES), whole(CHANS, HALF_LANES), whole(1, 1)],
        out_shape=[jax.ShapeDtypeStruct((2, 6, CHANS, 16, HALF_LANES), F32), jax.ShapeDtypeStruct((CHANS, HALF_LANES), F32),
                   jax.ShapeDtypeStruct((CHANS, HALF_LANES), F32), jax.ShapeDtypeStruct((1, 1), F32)],
        name="unpack",
    )(v.reshape(GROUPS, CHANS, CHANS, LANES), sm)
    return out.reshape(12, CHANS, 16, HALF_LANES), g1, g2.T, loss[0, 0]


def solution(mesh):
    w_size, h_size, dp_size = mesh.shape["w"], mesh.shape["h"], mesh.shape["dp"]
    fwd_np, inv_np = dft_tables(ROWS, HALF_LANES, w_size, h_size)

    def local_step(field, target, lat_weight, leg_fwd, leg_inv, spec_w, w_in, w_out):
        gf, gi = jnp.asarray(fwd_np), jnp.asarray(inv_np)
        packed, gs, sm = run_block(
            field, target, lat_weight, w_in, w_out.T, leg_fwd.transpose(0, 2, 1), leg_inv.transpose(0, 2, 1),
            spec_w.transpose(0, 2, 3, 1), gf, gi)
        d_field, grad_w_in, grad_w_out, loss = unpack(packed, sm)
        grad_spec = gs.reshape(2, 4, 2, 8, 4, CHANS).transpose(0, 3, 1, 2, 4, 5).reshape(2, 8, CHANS, CHANS)
        return loss, d_field, grad_spec, grad_w_in, grad_w_out

    grid_spec = P("dp", None, "h", "w")
    table_spec = P("w", None, "h")
    kernel_out = P(None, "h", None, None)
    return jax.shard_map(local_step, mesh=mesh, in_specs=(grid_spec, grid_spec, P("h"), table_spec, table_spec, P(), P(), P()), out_specs=(P(), grid_spec, kernel_out, P(), P()), check_vma=False)
```
